32 devices in a mesh: group: 2 (over x), serve: 8 (over z, y), tensor: 2 (over core).
Axes of the slice: x: 2, y: 2, z: 4, core: 2. Of those that a mesh axis runs over, the one named last changes fastest.
Arguments:
- tokens: bfloat16 [2048, 8192], P(('group', 'serve'), 'tensor'), parts along dimension 0, may hold values from -70 to 70
- query_weight: bfloat16 [8192, 512], P(None, 'tensor'), may hold values from -0.0625 to 0.0625
- key_value_weight: bfloat16 [8192, 256], P(None, 'tensor'), may hold values from -0.0625 to 0.0625
- output_weight: bfloat16 [512, 8192], P('tensor'), may hold values from -0.25 to 0.25
- adapter_down_maps: bfloat16 [32, 48, 8192], P(('group', 'serve'), None, 'tensor'), parts along dimension 0, may hold values from -0.0625 to 0.0625
- adapter_query_up: bfloat16 [32, 16, 512], P(('group', 'serve'), None, 'tensor'), parts along dimension 0, may hold values from -1.5 to 1.5
- adapter_key_value_up: bfloat16 [32, 16, 256], P(('group', 'serve'), None, 'tensor'), parts along dimension 0, may hold values from -1.5 to 1.5
- adapter_output_down: bfloat16 [32, 16, 512], P(('group', 'serve'), None, 'tensor'), parts along dimension 0, may hold values from -0.25 to 0.25
- adapter_output_up: bfloat16 [32, 16, 8192], P(('group', 'serve'), None, 'tensor'), parts along dimension 0, may hold values from -1.5 to 1.5
- request_adapter: int32 [16], P('group'), parts along dimension 0, may hold values from 0 to 15, as said below
- adapter_pool_row: int32 [32], P('group'), parts along dimension 0, may hold values from 0 to 15, as said below
- lengths: int32 [16], P(('group', 'serve')), parts along dimension 0, may hold values from 16 to 128
Outputs:
- attention_out: bfloat16 [2048, 8192], P(('group', 'serve'), 'tensor'), parts along dimension 0
The draws below stay inside these ranges and needn't reach their ends.
There are 2 independent parts, one for each index of `group`. The reference program is written for one: setup_inputs(seed, part) draws one part's arguments, and reference() takes and returns one part's arrays. A program takes and returns all parts, laid end to end along the dimension named above; an argument that names none is the same for every part. Nothing has to cross between parts.
Inputs may be any that keep to these rules, and one draw needn't show every extreme that they name: Grouping requests by adapter_pool_row[request_adapter[r]] // 2, no group holds more than 4 requests, and some group holds exactly 4. `adapter_pool_row`: each value appears once.
All inputs are finite; a program needn't handle non-finite values.
Results may differ from the reference program's by a relative error of at most 0.012.
The reference program's roundings to bfloat16 on the way count: a program that leaves them out, or rounds other values in their place, can miss the bound.
Values may be sent and summed in bfloat16 or wider, within the bound.
A program may use at most 128 MiB of HBM per device.

```python
import jax
import jax.numpy as jnp
from jax import lax

MODEL_WIDTH = 8192
HEAD_SIZE = 128
ADAPTER_RANK = 16
QUERY_HEADS = 4
CAP = 4
LEN = 128
ADP_DEV = 2
REQUESTS = 8
ADAPTER_POOL = 16
TOKENS = 1024


def draw_tokens(key, part):
    key_base = jax.random.fold_in(jax.random.fold_in(key, 11), 0)
    base_draw = jnp.clip(jax.random.normal(key_base, (TOKENS, MODEL_WIDTH), jnp.float32), -5.0, 5.0)
    return base_draw.astype(jnp.bfloat16)


def placement_draw(key):
    key_hot, key_seat, key_mix, key_local, key_slot = jax.random.split(jax.random.fold_in(key, 23), 5)
    seats_total = REQUESTS * CAP
    hot_owner = jax.random.randint(key_hot, (), 0, REQUESTS)
    seat_index = jnp.arange(seats_total, dtype=jnp.int32)
    seat_owner = seat_index // CAP
    scores = jax.random.permutation(key_seat, seats_total).astype(jnp.int32)
    scores = jnp.where(seat_owner == hot_owner, -1 - seat_index % CAP, scores)
    taken = jnp.argsort(scores, stable=True)[:REQUESTS]
    request_owner = jax.random.permutation(key_mix, seat_owner[taken])
    local_pick = jax.random.randint(key_local, (REQUESTS,), 0, ADP_DEV)
    wanted = request_owner * ADP_DEV + local_pick
    slot_table = jax.random.permutation(key_slot, ADAPTER_POOL).astype(jnp.int32)
    inverse = jnp.argsort(slot_table)
    return (slot_table, inverse[wanted].astype(jnp.int32))


def draw_request_adapter(key, part):
    return placement_draw(key)[1]


def draw_adapter_pool_row(key, part):
    return placement_draw(key)[0]


def touch_ends(array, key, low, top_value):
    longest = array.shape.index(max(array.shape))
    spots = []
    for shift in (0, 1):
        where = [jax.random.randint(jax.random.fold_in(key, axis), (), 0, length) for axis, length in enumerate(array.shape)]
        where[longest] = (where[longest] + shift) % array.shape[longest]
        spots.append(tuple(where))
    return array.at[spots[0]].set(low).at[spots[1]].set(top_value)


def levels(stream_key, dims, shards, smallest, top_value):
    loudness, own = 1.0, jax.random.fold_in(stream_key, 6)
    for position, shards_of in shards:
        heights = jnp.exp(jax.random.uniform(jax.random.fold_in(own, position), (shards_of,), jnp.float32, smallest / len(shards), top_value / len(shards)))
        loudness = loudness * jnp.repeat(heights, dims[position] // shards_of).reshape([-1 if axis == position else 1 for axis in range(len(dims))])
    return loudness


def bell_draw(own_key, extent, scale, bound, cuts=(), kind=jnp.bfloat16):
    array = jax.random.normal(own_key, extent, jnp.float32) * scale
    if len(cuts) > 0:
        array = levels(own_key, extent, cuts, -0.22, 0.18) * array
    return jnp.clip(array, min=-bound, max=bound).astype(kind)


def setup_inputs(seed: int = 0, part: int = 0) -> dict:
    streams_of = jax.random.split(jax.random.key(seed), 13)
    part_keys = jax.random.split(jax.random.fold_in(streams_of[12], part), 13)
    tokens = draw_tokens(jax.random.fold_in(jax.random.fold_in(streams_of[12], part), 71), part)
    query_weight = bell_draw(streams_of[1], (MODEL_WIDTH, QUERY_HEADS * HEAD_SIZE), MODEL_WIDTH ** -0.5, 0.0625, ((1, 2),))
    key_value_weight = bell_draw(streams_of[2], (MODEL_WIDTH, 2 * HEAD_SIZE), MODEL_WIDTH ** -0.5, 0.0625, ((1, 2),))
    output_weight = bell_draw(streams_of[3], (QUERY_HEADS * HEAD_SIZE, MODEL_WIDTH), (QUERY_HEADS * HEAD_SIZE) ** -0.5, 0.25, ((0, 2),))
    adapter_down_maps = bell_draw(part_keys[4], (ADAPTER_POOL, 3 * ADAPTER_RANK, MODEL_WIDTH), MODEL_WIDTH ** -0.5, 0.0625, ((0, 8), (2, 2)))
    adapter_query_up = bell_draw(part_keys[5], (ADAPTER_POOL, ADAPTER_RANK, QUERY_HEADS * HEAD_SIZE), ADAPTER_RANK ** -0.5, 1.5, ((0, 8), (2, 2)))
    adapter_key_value_up = bell_draw(part_keys[6], (ADAPTER_POOL, ADAPTER_RANK, 2 * HEAD_SIZE), ADAPTER_RANK ** -0.5, 1.5, ((0, 8), (2, 2)))
    adapter_output_down = bell_draw(part_keys[7], (ADAPTER_POOL, ADAPTER_RANK, QUERY_HEADS * HEAD_SIZE), (QUERY_HEADS * HEAD_SIZE) ** -0.5, 0.25, ((0, 8), (2, 2)))
    adapter_output_up = bell_draw(part_keys[8], (ADAPTER_POOL, ADAPTER_RANK, MODEL_WIDTH), ADAPTER_RANK ** -0.5, 1.5, ((0, 8), (2, 2)))
    request_adapter = draw_request_adapter(jax.random.fold_in(jax.random.fold_in(streams_of[12], part), 71), part)
    adapter_pool_row = draw_adapter_pool_row(jax.random.fold_in(jax.random.fold_in(streams_of[12], part), 71), part)
    lengths = touch_ends(jax.random.randint(part_keys[11], (REQUESTS,), LEN // 8, LEN + 1), jax.random.fold_in(part_keys[11], 1), LEN // 8, LEN).astype(jnp.int32)
    return {"tokens": tokens, "query_weight": query_weight, "key_value_weight": key_value_weight, "output_weight": output_weight, "adapter_down_maps": adapter_down_maps, "adapter_query_up": adapter_query_up, "adapter_key_value_up": adapter_key_value_up, "adapter_output_down": adapter_output_down, "adapter_output_up": adapter_output_up, "request_adapter": request_adapter, "adapter_pool_row": adapter_pool_row, "lengths": lengths}


def rotate(vectors):
    rows_count, width = vectors.shape
    half_width = width // 2
    freqs = 500000.0 ** (-(jnp.arange(half_width, dtype=jnp.float32) * 2.0 / width))
    angles = jnp.arange(rows_count, dtype=jnp.float32)[:, None] * freqs[None, :]
    cosine = jnp.cos(angles)
    sine_part = jnp.sin(angles)
    first = vectors[:, :half_width]
    second = vectors[:, half_width:]
    return jnp.concatenate([first * cosine - second * sine_part, second * cosine + first * sine_part], axis=1)


def attend(query_rows, key_rows, value_rows, length):
    rows_count = query_rows.shape[0]
    scores = jnp.dot(query_rows, key_rows.T, preferred_element_type=jnp.float32) * (query_rows.shape[1] ** -0.5)
    positions = jnp.arange(rows_count)
    allowed = (positions[None, :] <= positions[:, None]) & (positions[None, :] < length)
    scores = jnp.where(allowed, scores, -1e30)
    highest = jnp.max(scores, axis=1, keepdims=True)
    expo = jnp.exp(scores - highest)
    weights = (expo / jnp.sum(expo, axis=1, keepdims=True)).astype(jnp.bfloat16)
    return jnp.dot(weights, value_rows, preferred_element_type=jnp.float32).astype(jnp.bfloat16)


def reference(tokens, query_weight, key_value_weight, output_weight, adapter_down_maps, adapter_query_up, adapter_key_value_up, adapter_output_down, adapter_output_up, request_adapter, adapter_pool_row, lengths):
    heads = query_weight.shape[1] // HEAD_SIZE
    half_cols = heads * HEAD_SIZE // 2

    def one_request(request):
        x_rows = lax.dynamic_slice_in_dim(tokens, request * LEN, LEN, 0)
        pool_slot = adapter_pool_row[request_adapter[request]]
        down_map_rows = adapter_down_maps[pool_slot]
        query_up_map = adapter_query_up[pool_slot]
        key_value_up = adapter_key_value_up[pool_slot]
        output_down = adapter_output_down[pool_slot]
        output_up = adapter_output_up[pool_slot]
        length = lengths[request]
        shrink = jnp.dot(x_rows, down_map_rows.T, preferred_element_type=jnp.float32).astype(jnp.bfloat16)
        query_all = jnp.dot(x_rows, query_weight, preferred_element_type=jnp.float32) + jnp.dot(shrink[:, :ADAPTER_RANK], query_up_map, preferred_element_type=jnp.float32)
        key_part = jnp.dot(x_rows, key_value_weight[:, :HEAD_SIZE], preferred_element_type=jnp.float32) + jnp.dot(shrink[:, ADAPTER_RANK:2 * ADAPTER_RANK], key_value_up[:, :HEAD_SIZE], preferred_element_type=jnp.float32)
        value_part = jnp.dot(x_rows, key_value_weight[:, HEAD_SIZE:], preferred_element_type=jnp.float32) + jnp.dot(shrink[:, 2 * ADAPTER_RANK:3 * ADAPTER_RANK], key_value_up[:, HEAD_SIZE:], preferred_element_type=jnp.float32)
        key_rounded = lax.optimization_barrier(key_part.astype(jnp.bfloat16))
        key_rows = rotate(key_rounded.astype(jnp.float32)).astype(jnp.bfloat16)
        value_rows = value_part.astype(jnp.bfloat16)
        attended_list = []
        for head in range(heads):
            query_rows = rotate(query_all[:, head * HEAD_SIZE:(head + 1) * HEAD_SIZE]).astype(jnp.bfloat16)
            attended_list.append(attend(query_rows, key_rows, value_rows, length))
        attended_all = jnp.concatenate(attended_list, axis=1)
        base_total = jnp.zeros((LEN, MODEL_WIDTH), jnp.float32)
        for half in range(2):
            term = jnp.dot(attended_all[:, half * half_cols:(half + 1) * half_cols], output_weight[half * half_cols:(half + 1) * half_cols], preferred_element_type=jnp.float32)
            term = lax.optimization_barrier(term.astype(jnp.bfloat16))
            base_total = base_total + term.astype(jnp.float32)
        low = jnp.dot(attended_all, output_down.T, preferred_element_type=jnp.float32).astype(jnp.bfloat16)
        delta_out = jnp.dot(low, output_up, preferred_element_type=jnp.float32)
        valid_rows = (jnp.arange(LEN) < length)[:, None]
        return jnp.where(valid_rows, base_total + delta_out, 0.0).astype(jnp.bfloat16)

    results = lax.map(one_request, jnp.arange(REQUESTS, dtype=jnp.int32))
    return results.reshape(TOKENS, MODEL_WIDTH)
```

```python
import jax
import jax.numpy as jnp
from jax import lax
from jax.sharding import PartitionSpec as P

HEAD_SIZE = 128


def rotate(vectors):
    rows_count, width = vectors.shape
    half_width = width // 2
    freqs = 500000.0 ** (-(jnp.arange(half_width, dtype=jnp.float32) * 2.0 / width))
    angles = jnp.arange(rows_count, dtype=jnp.float32)[:, None] * freqs[None, :]
    cosine = jnp.cos(angles)
    sine_part = jnp.sin(angles)
    first = vectors[:, :half_width]
    second = vectors[:, half_width:]
    return jnp.concatenate(
        [first * cosine - second * sine_part, second * cosine + first * sine_part], axis=1
    )


def attend(query_rows, key_rows, value_rows, length):
    rows_count = query_rows.shape[0]
    scores = lax.dot_general(
        query_rows, key_rows, (((1,), (1,)), ((), ())), preferred_element_type=jnp.float32
    ) * query_rows.shape[1] ** (-0.5)
    positions = jnp.arange(rows_count)
    allowed = (positions[None, :] <= positions[:, None]) & (positions[None, :] < length)
    scores = jnp.where(allowed, scores, -1e30)
    highest = jnp.max(scores, axis=1, keepdims=True)
    expo = jnp.exp(scores - highest)
    weights = (expo / jnp.sum(expo, axis=1, keepdims=True)).astype(jnp.bfloat16)
    return jnp.dot(weights, value_rows, preferred_element_type=jnp.float32).astype(jnp.bfloat16)


def swap(x, axis, size, bit):
    return lax.ppermute(x, axis, [(i, i ^ bit) for i in range(size)])


def route(held, bits, size, server, wanted):
    count = held.shape[0]
    first_bit = bits[0]
    both = (held, swap(held, "serve", size, first_bit))

    def block_for(mask):
        target = wanted[server ^ mask]
        owner, slot = target // count, target % count
        near = ((owner ^ server) & first_bit) == 0
        pick = lambda member: lax.dynamic_index_in_dim(member, slot, 0, keepdims=False)
        return jnp.where(near, pick(both[0]), pick(both[1]))

    masks = [0]
    for bit in bits[1:]:
        masks = masks + [mask | bit for mask in masks]
    blocks = {mask: block_for(mask) for mask in masks}
    for bit in bits[1:]:
        kept = {}
        for mask in blocks:
            if mask & bit:
                continue
            arrived = swap(blocks[mask | bit], "serve", size, bit)
            owner = wanted[server ^ mask] // count
            kept[mask] = jnp.where(((owner ^ server) & bit) == 0, blocks[mask], arrived)
        blocks = kept
    return blocks[0]


def local(
    tokens,
    query_weight,
    key_value_weight,
    output_weight,
    adapter_down_maps,
    adapter_query_up,
    adapter_key_value_up,
    adapter_output_down,
    adapter_output_up,
    request_adapter,
    adapter_pool_row,
    lengths,
):
    server = lax.axis_index("serve")
    tensor_index = lax.axis_index("tensor")
    size = lax.axis_size("serve")
    low_rank = adapter_output_down.shape[1]
    half_width = tokens.shape[1]
    wanted = adapter_pool_row[request_adapter]

    other_tokens = swap(tokens, "tensor", 2, 1)
    out_width = output_weight.shape[1] // 2
    own_cols = lax.dynamic_slice_in_dim(output_weight, tensor_index * out_width, out_width, 1)
    sent_cols = lax.dynamic_slice_in_dim(output_weight, (1 - tensor_index) * out_width, out_width, 1)
    other_rows_weight = swap(sent_cols, "tensor", 2, 1)

    small_width = max(adapter_query_up.shape[2], adapter_key_value_up.shape[2], adapter_output_down.shape[2])
    widen = lambda m: jnp.pad(m, ((0, 0), (0, 0), (0, small_width - m.shape[2])))
    small = jnp.concatenate(
        [widen(adapter_query_up), widen(adapter_key_value_up), widen(adapter_output_down)], axis=1
    )
    bits = []
    while 2 ** len(bits) < size:
        bits.append(2 ** len(bits))
    turned = bits[1::-1] + bits[2:]
    cut = half_width // 2
    first = route(jnp.concatenate([adapter_down_maps[:, :, :cut], small], axis=2), bits, size, server, wanted)
    second = route(adapter_down_maps[:, :, cut:], turned, size, server, wanted)
    output_up = route(adapter_output_up, turned, size, server, wanted)
    query_up_map = first[:low_rank, cut : cut + adapter_query_up.shape[2]]
    key_value_up = first[low_rank : 2 * low_rank, cut : cut + adapter_key_value_up.shape[2]]
    output_down = first[2 * low_rank :, cut : cut + adapter_output_down.shape[2]]

    def times(weight):
        own = lax.dynamic_slice_in_dim(weight, tensor_index * half_width, half_width, 0)
        other = lax.dynamic_slice_in_dim(weight, (1 - tensor_index) * half_width, half_width, 0)
        return jnp.dot(tokens, own, preferred_element_type=jnp.float32) + jnp.dot(
            other_tokens, other, preferred_element_type=jnp.float32
        )

    query_base = times(query_weight)
    pair_base = times(key_value_weight)
    contract = lambda x, m: lax.dot_general(
        x, m, (((1,), (1,)), ((), ())), preferred_element_type=jnp.float32
    )
    partial_shrink = contract(tokens[:, :cut], first[:, :cut]) + contract(tokens[:, cut:], second)
    shrink = (partial_shrink + swap(partial_shrink, "tensor", 2, 1)).astype(jnp.bfloat16)
    pair_shrink = jnp.where(
        tensor_index == 0, shrink[:, low_rank : 2 * low_rank], shrink[:, 2 * low_rank :]
    )
    own_part = (
        pair_base + jnp.dot(pair_shrink, key_value_up, preferred_element_type=jnp.float32)
    ).astype(jnp.bfloat16)
    other_part = swap(own_part, "tensor", 2, 1)
    query_all = query_base + jnp.dot(
        shrink[:, :low_rank], query_up_map, preferred_element_type=jnp.float32
    )
    key_part = jnp.where(tensor_index == 0, own_part, other_part)
    value_rows = jnp.where(tensor_index == 0, other_part, own_part)
    key_rows = rotate(key_part.astype(jnp.float32)).astype(jnp.bfloat16)
    heads_here = query_weight.shape[1] // HEAD_SIZE
    attended_list = []
    for head in range(heads_here):
        query_rows = rotate(query_all[:, head * HEAD_SIZE : (head + 1) * HEAD_SIZE]).astype(
            jnp.bfloat16
        )
        attended_list.append(attend(query_rows, key_rows, value_rows, lengths[0]))
    attended = jnp.concatenate(attended_list, axis=1)
    other_attended = swap(attended, "tensor", 2, 1)
    partial_low = contract(attended, output_down)
    low_out = (partial_low + swap(partial_low, "tensor", 2, 1)).astype(jnp.bfloat16)
    own_term = jnp.dot(attended, own_cols, preferred_element_type=jnp.float32).astype(jnp.bfloat16)
    other_term = jnp.dot(
        other_attended, other_rows_weight, preferred_element_type=jnp.float32
    ).astype(jnp.bfloat16)
    base_out = own_term.astype(jnp.float32) + other_term.astype(jnp.float32)
    delta_out = jnp.dot(low_out, output_up, preferred_element_type=jnp.float32)
    valid_rows = (jnp.arange(tokens.shape[0]) < lengths[0])[:, None]
    return jnp.where(valid_rows, base_out + delta_out, 0.0).astype(jnp.bfloat16)


def solution(mesh):
    placed = (
        P(("group", "serve"), "tensor"),
        P(None, "tensor"),
        P(None, "tensor"),
        P("tensor", None),
        P(("group", "serve"), None, "tensor"),
        P(("group", "serve"), None, "tensor"),
        P(("group", "serve"), None, "tensor"),
        P(("group", "serve"), None, "tensor"),
        P(("group", "serve"), None, "tensor"),
        P("group"),
        P("group"),
        P(("group", "serve")),
    )
    return jax.shard_map(
        local,
        mesh=mesh,
        in_specs=placed,
        out_specs=P(("group", "serve"), "tensor"),
        check_vma=False,
    )
```

```python
import jax
import jax.numpy as jnp
from jax import lax
from jax.sharding import PartitionSpec as P

HEAD_SIZE = 128


def rotate(vectors):
    rows_count, width = vectors.shape
    half_width = width // 2
    freqs = 500000.0 ** (-(jnp.arange(half_width, dtype=jnp.float32) * 2.0 / width))
    angles = jnp.arange(rows_count, dtype=jnp.float32)[:, None] * freqs[None, :]
    cosine = jnp.cos(angles)
    sine_part = jnp.sin(angles)
    first = vectors[:, :half_width]
    second = vectors[:, half_width:]
    return jnp.concatenate(
        [first * cosine - second * sine_part, second * cosine + first * sine_part], axis=1
    )


def attend(query_rows, key_rows, value_rows, length):
    rows_count = query_rows.shape[0]
    scores = lax.dot_general(
        query_rows, key_rows, (((1,), (1,)), ((), ())), preferred_element_type=jnp.float32
    ) * query_rows.shape[1] ** (-0.5)
    positions = jnp.arange(rows_count)
    allowed = (positions[None, :] <= positions[:, None]) & (positions[None, :] < length)
    scores = jnp.where(allowed, scores, -1e30)
    highest = jnp.max(scores, axis=1, keepdims=True)
    expo = jnp.exp(scores - highest)
    weights = (expo / jnp.sum(expo, axis=1, keepdims=True)).astype(jnp.bfloat16)
    return jnp.dot(weights, value_rows, preferred_element_type=jnp.float32).astype(jnp.bfloat16)


def swap(x, axis, size, bit):
    return lax.ppermute(x, axis, [(i, i ^ bit) for i in range(size)])


def route(held, bits, size, server, wanted):
    count = held.shape[0]
    first_bit = bits[0]
    both = (held, swap(held, "serve", size, first_bit))

    def block_for(mask):
        target = wanted[server ^ mask]
        owner, slot = target // count, target % count
        near = ((owner ^ server) & first_bit) == 0
        pick = lambda member: lax.dynamic_index_in_dim(member, slot, 0, keepdims=False)
        return jnp.where(near, pick(both[0]), pick(both[1]))

    masks = [0]
    for bit in bits[1:]:
        masks = masks + [mask | bit for mask in masks]
    blocks = {mask: block_for(mask) for mask in masks}
    for bit in bits[1:]:
        kept = {}
        for mask in blocks:
            if mask & bit:
                continue
            arrived = swap(blocks[mask | bit], "serve", size, bit)
            owner = wanted[server ^ mask] // count
            kept[mask] = jnp.where(((owner ^ server) & bit) == 0, blocks[mask], arrived)
        blocks = kept
    return blocks[0]


def local(
    tokens,
    query_weight,
    key_value_weight,
    output_weight,
    adapter_down_maps,
    adapter_query_up,
    adapter_key_value_up,
    adapter_output_down,
    adapter_output_up,
    request_adapter,
    adapter_pool_row,
    lengths,
):
    server = lax.axis_index("serve")
    tensor_index = lax.axis_index("tensor")
    size = lax.axis_size("serve")
    low_rank = adapter_output_down.shape[1]
    half_width = tokens.shape[1]
    wanted = adapter_pool_row[request_adapter]

    other_tokens = swap(tokens, "tensor", 2, 1)
    out_width = output_weight.shape[1] // 2

    small_width = max(adapter_query_up.shape[2], adapter_key_value_up.shape[2], adapter_output_down.shape[2])
    widen = lambda m: jnp.pad(m, ((0, 0), (0, 0), (0, small_width - m.shape[2])))
    small = jnp.concatenate(
        [widen(adapter_query_up), widen(adapter_key_value_up), widen(adapter_output_down)], axis=1
    )
    bits = []
    while 2 ** len(bits) < size:
        bits.append(2 ** len(bits))
    turned = bits[1::-1] + bits[2:]
    cut = half_width // 2
    first = route(jnp.concatenate([adapter_down_maps[:, :, :cut], small], axis=2), bits, size, server, wanted)
    second = route(adapter_down_maps[:, :, cut:], turned, size, server, wanted)
    output_up = route(adapter_output_up, turned, size, server, wanted)
    query_up_map = first[:low_rank, cut : cut + adapter_query_up.shape[2]]
    key_value_up = first[low_rank : 2 * low_rank, cut : cut + adapter_key_value_up.shape[2]]
    output_down = first[2 * low_rank :, cut : cut + adapter_output_down.shape[2]]

    def times(weight):
        own = lax.dynamic_slice_in_dim(weight, tensor_index * half_width, half_width, 0)
        other = lax.dynamic_slice_in_dim(weight, (1 - tensor_index) * half_width, half_width, 0)
        return jnp.dot(tokens, own, preferred_element_type=jnp.float32) + jnp.dot(
            other_tokens, other, preferred_element_type=jnp.float32
        )

    query_base = times(query_weight)
    pair_base = times(key_value_weight)
    contract = lambda x, m: lax.dot_general(
        x, m, (((1,), (1,)), ((), ())), preferred_element_type=jnp.float32
    )
    partial_shrink = contract(tokens[:, :cut], first[:, :cut]) + contract(tokens[:, cut:], second)
    shrink = (partial_shrink + swap(partial_shrink, "tensor", 2, 1)).astype(jnp.bfloat16)
    pair_shrink = jnp.where(
        tensor_index == 0, shrink[:, low_rank : 2 * low_rank], shrink[:, 2 * low_rank :]
    )
    own_part = (
        pair_base + jnp.dot(pair_shrink, key_value_up, preferred_element_type=jnp.float32)
    ).astype(jnp.bfloat16)
    other_part = swap(own_part, "tensor", 2, 1)
    query_all = query_base + jnp.dot(
        shrink[:, :low_rank], query_up_map, preferred_element_type=jnp.float32
    )
    key_part = jnp.where(tensor_index == 0, own_part, other_part)
    value_rows = jnp.where(tensor_index == 0, other_part, own_part)
    key_rows = rotate(key_part.astype(jnp.float32)).astype(jnp.bfloat16)
    heads_here = query_weight.shape[1] // HEAD_SIZE
    attended_list = []
    for head in range(heads_here):
        query_rows = rotate(query_all[:, head * HEAD_SIZE : (head + 1) * HEAD_SIZE]).astype(
            jnp.bfloat16
        )
        attended_list.append(attend(query_rows, key_rows, value_rows, lengths[0]))
    attended = jnp.concatenate(attended_list, axis=1)
    partial_low = contract(attended, output_down)
    low_out = (partial_low + swap(partial_low, "tensor", 2, 1)).astype(jnp.bfloat16)
    def term(start, width):
        cols = lax.dynamic_slice_in_dim(output_weight, start, width, 1)
        return jnp.dot(attended, cols, preferred_element_type=jnp.float32).astype(jnp.bfloat16)

    piece = out_width // 2
    other_start = (1 - tensor_index) * out_width
    arrived = [swap(term(other_start + i * piece, piece), "tensor", 2, 1) for i in range(2)]
    own_term = term(tensor_index * out_width, out_width)
    other_term = jnp.concatenate(arrived, axis=1)
    base_out = own_term.astype(jnp.float32) + other_term.astype(jnp.float32)
    delta_out = jnp.dot(low_out, output_up, preferred_element_type=jnp.float32)
    valid_rows = (jnp.arange(tokens.shape[0]) < lengths[0])[:, None]
    return jnp.where(valid_rows, base_out + delta_out, 0.0).astype(jnp.bfloat16)


def solution(mesh):
    placed = (
        P(("group", "serve"), "tensor"),
        P(None, "tensor"),
        P(None, "tensor"),
        P("tensor", None),
        P(("group", "serve"), None, "tensor"),
        P(("group", "serve"), None, "tensor"),
        P(("group", "serve"), None, "tensor"),
        P(("group", "serve"), None, "tensor"),
        P(("group", "serve"), None, "tensor"),
        P("group"),
        P("group"),
        P(("group", "serve")),
    )
    return jax.shard_map(
        local,
        mesh=mesh,
        in_specs=placed,
        out_specs=P(("group", "serve"), "tensor"),
        check_vma=False,
    )
```
